256 devices in a mesh: gz: 16 (over y_lo, z), ang: 16 (over x, y_hi, core).
Axes of the slice: x: 4, y: 4 (y_hi: 2, y_lo: 2; y = y_hi * 2 + y_lo), z: 8, core: 2. Of those that a mesh axis runs over, the one named last changes fastest.
Arguments:
- fan_views: bfloat16 [16, 64, 128, 896], P('gz', None, 'ang'), may hold values from -6 to 6
- rebin_weight: bfloat16 [896, 896], replicated, may hold values from -0.1875 to 0.1875
- slab_table: int32 [16, 16, 1], P('gz'), may hold values from 0 to 15; in each aligned block of 16 rows (0 to 15, 16 to 31, ..., all dimensions but the last counted through in order) at most 2 rows name the same one
- slice_offset: int32 [16, 16], P('gz'), may hold values from 0 to 60
- tiles: bfloat16 [2048, 896, 128], P('ang'), may hold values from -0.015625 to 0.015625
- tile_view: int32 [2048], P('ang'), may hold values from 0 to 7, as said below
Outputs:
- volume: float32 [512, 2048], P(('gz', 'ang'))
The draws below stay inside these ranges and needn't reach their ends.
Inputs may be any that keep to these rules, and one draw needn't show every extreme that they name: `slab_table`: entry [t, b, 0] is the slab receiving row block b of turn t; one turn sends at most 2 row blocks to one slab. `tile_view`: the 8 entries of each aligned run (one angle group and one pixel block) are a permutation of 0 to 7.
All inputs are finite; a program needn't handle non-finite values.
Results may differ from the reference program's by a relative error of at most 0.0059.
Values may be sent and summed in bfloat16 or wider, within the bound.
A program may use at most 128 MiB of HBM per device.

```python
import math
import jax
import jax.numpy as jnp
import numpy as np
from jax import lax

COLS = 896
ROWS = 64
BR = 4
CAP = 2
HALO = 16
TILE_PIX = 128
VIEWS_DEV = 8
PIX = 2048
ZD = 32
TURNS = 16
BLOCKS = 16
VIEWS = 128
PIXBLK = 16
TILE_DEV = 128
NTILES = 2048
ZE = 64
NZ = 512
N_GZ = 16


def shuffle_views(subkey):
    return jax.random.permutation(subkey, VIEWS_DEV)


def draw_tile_view(key, part):
    group_count = NTILES // VIEWS_DEV
    subkeys = jax.random.split(key, group_count)
    orders = jax.vmap(shuffle_views)(subkeys)
    return orders.reshape(NTILES).astype(jnp.int32)


def set_ends(entries, stream_key, least, top_value):
    longest = entries.shape.index(max(entries.shape))
    spots = []
    for shift in (0, 1):
        where = [jax.random.randint(jax.random.fold_in(stream_key, axis), (), 0, length) for axis, length in enumerate(entries.shape)]
        where[longest] = (where[longest] + shift) % entries.shape[longest]
        spots.append(tuple(where))
    return entries.at[spots[0]].set(least).at[spots[1]].set(top_value)


def block_levels(stream_key, extent, shards, low, top_value):
    loudness, own = 1.0, jax.random.fold_in(stream_key, 6)
    for dim, blocks in shards:
        draws = jnp.exp(jax.random.uniform(jax.random.fold_in(own, dim), (blocks,), jnp.float32, low / len(shards), top_value / len(shards)))
        loudness = loudness * jnp.repeat(draws, extent[dim] // blocks).reshape([-1 if axis == dim else 1 for axis in range(len(extent))])
    return loudness


def deal_out(own_key, own, number, rows, amount, top, most, lean):
    ranking = jax.random.permutation(own_key, amount)
    crowded, usual = portions_of(amount, rows * top, most, lean, True), portions_of(amount, rows * top, most, lean, False)
    places = jnp.arange(amount)

    def named(tallies, offset_by):
        used = int((tallies > 0).sum())
        fixed = max(1, used // 4)
        moved = fixed + (places - fixed + offset_by * (used - fixed)) % max(1, amount - fixed)
        return jnp.zeros((amount,), jnp.int32).at[ranking[jnp.where(places < fixed, places, moved)]].set(jnp.asarray(tallies, jnp.int32))

    tallies = jnp.where(number % 4 == 0, named(crowded, number // 4), named(usual, number - number // 4 - 1))
    mixed = jax.random.permutation(jax.random.fold_in(own, 3), amount)
    source_of, taker = mixed[0:amount // 2 * 2:2], mixed[1:amount // 2 * 2:2]
    margin = jnp.minimum(tallies[source_of] - 1, most - tallies[taker]) // 2
    margin = jnp.where((source_of == ranking[0]) | (taker == ranking[0]) | (tallies[taker] == 0), 0, jnp.maximum(margin, 0))
    moved = jax.random.randint(jax.random.fold_in(own, 4), (amount // 2,), 0, 1 << 20) % (margin + 1)
    tallies = tallies.at[source_of].add(-moved).at[taker].add(moved)
    items = jnp.searchsorted(jnp.cumsum(tallies), jnp.arange(rows * top), side="right").astype(jnp.int32)
    table = items.reshape(top, rows).T
    table = table[jax.random.permutation(jax.random.fold_in(own, 1), rows)]
    offset_by = jax.random.randint(jax.random.fold_in(own, 2), (rows, 1), 0, top)
    return jnp.take_along_axis(table, (jnp.arange(top)[None, :] + offset_by) % top, axis=1)


def portions_of(amount, total, bound, lean, full):
    loads = [(1 << 20) // math.isqrt(standing ** lean) + 1 for standing in range(1, amount + 1)]
    largest = bound if full else min(bound, max(-(-total // amount), total * loads[0] // sum(loads)))
    least = 1 if total - largest >= amount - 1 else 0
    holding, spare = [largest] + [least] * (amount - 1), total - largest - least * (amount - 1)
    while spare > 0:
        candidates = [i for i in range(1, amount) if holding[i] < largest] or [i for i in range(1, amount) if holding[i] < bound]
        whole, budget = sum([loads[i] for i in candidates]), spare
        for i in candidates:
            more = min(bound - holding[i], max(1, budget * loads[i] // whole), spare)
            holding[i] = holding[i] + more
            spare = spare - more
    return np.array(holding)


def noise(rng, dims, spread, limit, cuts=(), held_as=jnp.bfloat16):
    values = jax.random.normal(rng, dims, jnp.float32) * spread
    if len(cuts) > 0:
        values = block_levels(rng, dims, cuts, -0.22, 0.18) * values
    return jnp.clip(values, min=-limit, max=limit).astype(held_as)


def setup_inputs(seed: int = 0) -> dict:
    arg_keys = jax.random.split(jax.random.key(seed), 7)
    fan_views = noise(arg_keys[0], (TURNS, ROWS, VIEWS, COLS), 1.0, 6.0, ((0, 16), (2, 16)))
    rebin_weight = noise(arg_keys[1], (COLS, COLS), COLS ** -0.5, 0.1875)
    slab_table_keys = jax.random.split(jax.random.fold_in(arg_keys[2], 1), TURNS * BLOCKS // BLOCKS)
    slab_table_turns = jax.random.permutation(jax.random.fold_in(arg_keys[2], 3), TURNS * BLOCKS // BLOCKS)
    slab_table = jax.vmap(lambda own, number: deal_out(jax.random.fold_in(arg_keys[2], 2), own, number, BLOCKS, N_GZ, 1, CAP, 2))(slab_table_keys, slab_table_turns).reshape((TURNS, BLOCKS, 1))
    slice_offset = set_ends(jax.random.randint(arg_keys[3], (TURNS, BLOCKS), 0, ZE - BR + 1), jax.random.fold_in(arg_keys[3], 1), 0, ZE - BR).astype(jnp.int32)
    tiles = noise(arg_keys[4], (NTILES, COLS, TILE_PIX), (VIEWS * COLS) ** -0.5, 0.015625, ((0, 16),))
    tile_view = draw_tile_view(jax.random.fold_in(arg_keys[6], 71), 0)
    return {"fan_views": fan_views, "rebin_weight": rebin_weight, "slab_table": slab_table, "slice_offset": slice_offset, "tiles": tiles, "tile_view": tile_view}


def filter_tables(columns):
    column_index = jnp.arange(columns, dtype=jnp.int32)
    phase_steps = (column_index[:, None] * column_index[None, :]) % columns
    radians = phase_steps.astype(jnp.float32) * (2.0 * math.pi / columns)
    dft_table = jnp.concatenate([jnp.cos(radians), jnp.sin(radians)], axis=1).astype(jnp.bfloat16)
    frequency = jnp.minimum(column_index, columns - column_index).astype(jnp.float32) * (2.0 / (columns * columns))
    ramp_weight = jnp.concatenate([frequency, frequency])
    return dft_table, ramp_weight


def ramp_filter(values, dft_table, ramp_weight):
    spectrum = jnp.dot(values, dft_table, preferred_element_type=jnp.float32)
    weighted = (spectrum * ramp_weight).astype(jnp.bfloat16)
    result = lax.dot_general(weighted, dft_table, (((1,), (1,)), ((), ())), preferred_element_type=jnp.float32)
    return result.astype(jnp.bfloat16)


def reference(fan_views, rebin_weight, slab_table, slice_offset, tiles, tile_view):
    dft_table, ramp_weight = filter_tables(COLS)
    group_count = NTILES // TILE_DEV
    global_view = (jnp.arange(NTILES, dtype=jnp.int32) // TILE_DEV) * VIEWS_DEV + tile_view.astype(jnp.int32)
    view_index = global_view.reshape(group_count, PIXBLK, VIEWS_DEV).transpose(1, 0, 2).reshape(PIXBLK, VIEWS)
    weights = tiles.reshape(group_count, PIXBLK, VIEWS_DEV * COLS, TILE_PIX).transpose(1, 0, 2, 3)
    weights = weights.reshape(PIXBLK, VIEWS * COLS, TILE_PIX)
    row_block = jnp.arange(ROWS, dtype=jnp.int32) // BR
    row_within = jnp.arange(ROWS, dtype=jnp.int32) % BR

    def one_turn(volume, inputs):
        fan_turn, slab_turn, offset_turn = inputs
        parallel = jnp.dot(fan_turn.reshape(ROWS * VIEWS, COLS), rebin_weight, preferred_element_type=jnp.float32).astype(jnp.bfloat16)
        filtered = ramp_filter(parallel, dft_table, ramp_weight).reshape(ROWS, VIEWS, COLS)
        pieces = []
        for pixel_block in range(PIXBLK):
            chosen = jnp.take(filtered, view_index[pixel_block], axis=1).reshape(ROWS, VIEWS * COLS)
            pieces.append(jnp.dot(chosen, weights[pixel_block], preferred_element_type=jnp.float32))
        back = jnp.concatenate(pieces, axis=1)
        global_depth = slab_turn[row_block, 0].astype(jnp.int32) * ZD + offset_turn[row_block].astype(jnp.int32) - HALO + row_within
        global_depth = jnp.where((global_depth >= 0) & (global_depth < NZ), global_depth, NZ).astype(jnp.int32)
        volume = volume.at[global_depth].add(back, mode="drop")
        return volume, None

    start_volume = jnp.zeros((NZ, PIX), jnp.float32)
    volume, _ = lax.scan(one_turn, start_volume, (fan_views, slab_table, slice_offset))
    return volume
```

```python
import functools
import math

import jax
import jax.numpy as jnp
import ml_dtypes
import numpy as np
from jax import lax
from jax.experimental import pallas as pl
from jax.experimental.pallas import tpu as pltpu
from jax.sharding import PartitionSpec as P

BR = 4
TILE_PIX = 128
F32, BF16 = jnp.float32, jnp.bfloat16


def filter_operator(columns):
    index = np.arange(columns)
    radians = (index[:, None] * index[None, :] % columns).astype(np.float64) * (2.0 * math.pi / columns)
    table = np.concatenate([np.cos(radians), np.sin(radians)], axis=1)
    table = table.astype(np.float32).astype(ml_dtypes.bfloat16).astype(np.float64)
    frequency = np.minimum(index, columns - index) * (2.0 / (columns * columns))
    ramp = np.concatenate([frequency, frequency])
    return ((table * ramp) @ table.T).astype(np.float32).astype(ml_dtypes.bfloat16)


def kernel(
    n_gz, n_ang,
    slab_ref, offset_ref, view_ref, fan_hbm, rebin_hbm, filter_hbm, tiles_hbm,
    out_ref,
    fan_v, rebin_v, filter_v, tiles_v, par_v, filt_v, place_v,
    send1, recv1, send2, recv2, send3, recv3,
    in_sem, tile_sem, s1, r1, s2, r2, s3, r3,
):
    gz, ang = lax.axis_index("gz"), lax.axis_index("ang")
    blocks, views, rows, cols = n_ang, fan_v.shape[1], fan_v.shape[0], fan_v.shape[2]
    zd = send2.shape[1]
    total_z = n_gz * zd

    def ang_peer(d):
        return lax.rem(ang + d, n_ang)

    def gz_peer(d):
        return lax.rem(gz + d, n_gz)

    loads = [
        pltpu.make_async_copy(fan_hbm.at[0], fan_v, in_sem.at[0]),
        pltpu.make_async_copy(rebin_hbm, rebin_v, in_sem.at[1]),
        pltpu.make_async_copy(filter_hbm, filter_v, in_sem.at[2]),
    ]
    for load in loads:
        load.start()

    def tile_load(i):
        return pltpu.make_async_copy(
            tiles_hbm.at[pl.ds(ang_peer(i + 1) * views, views)],
            tiles_v.at[pl.ds(i * views, views)],
            tile_sem.at[i],
        )

    def start_tile(i, carry):
        tile_load(i).start()
        return carry

    lax.fori_loop(0, blocks, start_tile, 0)

    barrier = pltpu.get_barrier_semaphore()
    for d in range(1, n_ang):
        pl.semaphore_signal(barrier, inc=1, device_id={"ang": ang_peer(d)}, device_id_type=pl.DeviceIdType.MESH)
    for d in range(1, n_gz):
        pl.semaphore_signal(barrier, inc=1, device_id={"gz": gz_peer(d)}, device_id_type=pl.DeviceIdType.MESH)

    lane = lax.broadcasted_iota(jnp.int32, (1, 2 * rows), 1)
    lane = lax.rem(lane, rows)
    depth = jnp.full((1, 2 * rows), -1, jnp.int32)
    for b in range(rows // BR):
        first = slab_ref[0, b] * zd + offset_ref[0, b] - zd // 2
        depth = jnp.where(lane // BR == b, first + lax.rem(lane, BR), depth)
    slices = lax.broadcasted_iota(jnp.int32, (total_z, 2 * rows), 0)
    place_v[...] = jnp.where(slices == depth, 1.0, 0.0).astype(BF16)

    loads[0].wait()
    loads[1].wait()
    par = jnp.dot(fan_v[...].reshape(rows * views, cols), rebin_v[...], preferred_element_type=F32)
    for c in range(cols // 128):
        par_v[c * rows * views : (c + 1) * rows * views] = par[:, c * 128 : (c + 1) * 128]
    loads[2].wait()
    by_view = jnp.concatenate(
        [
            jnp.concatenate(
                [par_v[pl.ds(c * rows * views + v, rows, stride=views)].astype(BF16) for c in range(cols // 128)],
                axis=1,
            )
            for v in range(views)
        ],
        axis=0,
    )
    filtered = jnp.dot(by_view, filter_v[...], preferred_element_type=F32).astype(BF16)
    filt_v[...] = filtered.reshape(views, rows, cols)

    pl.semaphore_wait(barrier, n_ang + n_gz - 2)

    def send_partial(i):
        to = ang_peer(i + 1)
        return pltpu.make_async_remote_copy(
            src_ref=send1.at[i], dst_ref=recv1.at[ang], send_sem=s1.at[i], recv_sem=r1.at[ang],
            device_id={"ang": to}, device_id_type=pl.DeviceIdType.MESH,
        )

    def pair(k, carry):
        a, b = 2 * k, 2 * k + 1
        tile_load(a).wait()
        tile_load(b).wait()
        acc = jnp.zeros((2 * rows, 2 * TILE_PIX), F32)
        for j in range(0, views, 2):
            lhs = jnp.concatenate(
                [
                    jnp.concatenate(
                        [filt_v[view_ref[ang_peer(x + 1) * views + j + h]] for h in range(2)], axis=1
                    )
                    for x in (a, b)
                ],
                axis=0,
            )
            rhs = jnp.concatenate(
                [
                    jnp.concatenate([tiles_v[x * views + j + h] for h in range(2)], axis=0)
                    for x in (a, b)
                ],
                axis=1,
            )
            acc = acc + jnp.dot(lhs, rhs, preferred_element_type=F32)
        send1[a] = acc[:rows, :TILE_PIX].astype(BF16)
        send1[b] = acc[rows:, TILE_PIX:].astype(BF16)
        send_partial(a).start()

        @pl.when(b < blocks - 1)
        def _():
            send_partial(b).start()

        return carry

    lax.fori_loop(0, blocks // 2, pair, 0)

    def wait_recv(buffer, sem, index, axis):
        pltpu.make_async_remote_copy(
            src_ref=buffer.at[index], dst_ref=buffer.at[index], send_sem=sem.at[index], recv_sem=sem.at[index],
            device_id={axis: index}, device_id_type=pl.DeviceIdType.MESH,
        ).wait_recv()

    for d in range(1, n_ang):
        wait_recv(recv1, r1, ang_peer(d), "ang")
    total = send1[blocks - 1].astype(F32)
    for d in range(1, n_ang):
        total = total + recv1[ang_peer(d)].astype(F32)
    high = total.astype(BF16)
    low = (total - high.astype(F32)).astype(BF16)
    placed = jnp.dot(place_v[...], jnp.concatenate([high, low], axis=0), preferred_element_type=F32)
    send2[...] = placed.astype(BF16).reshape(n_gz, zd, TILE_PIX)

    def send_slab(d):
        to = gz_peer(d)
        return pltpu.make_async_remote_copy(
            src_ref=send2.at[to], dst_ref=recv2.at[gz], send_sem=s2.at[to], recv_sem=r2.at[gz],
            device_id={"gz": to}, device_id_type=pl.DeviceIdType.MESH,
        )

    for d in range(1, n_gz):
        send_slab(d).start()
    slab = send2[gz].astype(F32)
    for d in range(1, n_gz):
        wait_recv(recv2, r2, gz_peer(d), "gz")
    for d in range(1, n_gz):
        slab = slab + recv2[gz_peer(d)].astype(F32)

    send3[...] = slab.reshape(n_ang, 2, TILE_PIX)

    def send_slices(d):
        to = ang_peer(d)
        return pltpu.make_async_remote_copy(
            src_ref=send3.at[to], dst_ref=recv3.at[ang], send_sem=s3.at[to], recv_sem=r3.at[ang],
            device_id={"ang": to}, device_id_type=pl.DeviceIdType.MESH,
        )

    for d in range(1, n_ang):
        send_slices(d).start()
    recv3[ang] = send3[ang]
    for d in range(1, n_ang):
        wait_recv(recv3, r3, ang_peer(d), "ang")
    for p in range(blocks):
        out_ref[:, p * TILE_PIX : (p + 1) * TILE_PIX] = recv3[p]

    for i in range(blocks - 1):
        send_partial(i).wait_send()
    for d in range(1, n_gz):
        send_slab(d).wait_send()
    for d in range(1, n_ang):
        send_slices(d).wait_send()


def on_device(n_gz, n_ang, fan_views, rebin_weight, slab_table, slice_offset, tiles, tile_view):
    _, rows, views, cols = fan_views.shape
    zd = 2 * n_ang
    operator = jnp.asarray(filter_operator(cols))
    dma = pltpu.SemaphoreType.DMA
    smem, hbm = pl.BlockSpec(memory_space=pltpu.SMEM), pl.BlockSpec(memory_space=pl.ANY)
    return pl.pallas_call(
        functools.partial(kernel, n_gz, n_ang),
        out_shape=jax.ShapeDtypeStruct((2, n_ang * TILE_PIX), F32),
        in_specs=[smem, smem, smem, hbm, hbm, hbm, hbm],
        out_specs=pl.BlockSpec(memory_space=pltpu.VMEM),
        scratch_shapes=[
            pltpu.VMEM((rows, views, cols), BF16),
            pltpu.VMEM((cols, cols), BF16),
            pltpu.VMEM((cols, cols), BF16),
            pltpu.VMEM((n_ang * views, cols, TILE_PIX), BF16),
            pltpu.VMEM((cols // 128 * rows * views, 128), F32),
            pltpu.VMEM((views, rows, cols), BF16),
            pltpu.VMEM((n_gz * zd, 2 * rows), BF16),
            pltpu.VMEM((n_ang, rows, TILE_PIX), BF16),
            pltpu.VMEM((n_ang, rows, TILE_PIX), BF16),
            pltpu.VMEM((n_gz, zd, TILE_PIX), BF16),
            pltpu.VMEM((n_gz, zd, TILE_PIX), BF16),
            pltpu.VMEM((n_ang, 2, TILE_PIX), F32),
            pltpu.VMEM((n_ang, 2, TILE_PIX), F32),
            dma((3,)),
            dma((n_ang,)),
            dma((n_ang,)), dma((n_ang,)),
            dma((n_gz,)), dma((n_gz,)),
            dma((n_ang,)), dma((n_ang,)),
        ],
        compiler_params=pltpu.CompilerParams(
            collective_id=0, has_side_effects=True, vmem_limit_bytes=60 * 1024 * 1024
        ),
        name="reconstruct",
    )(slab_table[:, :, 0], slice_offset, tile_view, fan_views, rebin_weight, operator, tiles)


def solution(mesh):
    n_gz, n_ang = mesh.shape["gz"], mesh.shape["ang"]
    in_specs = (
        P("gz", None, "ang", None),
        P(),
        P("gz", None, None),
        P("gz", None),
        P("ang", None, None),
        P("ang"),
    )
    out_specs = P(("gz", "ang"), None)
    return jax.shard_map(
        functools.partial(on_device, n_gz, n_ang),
        mesh=mesh, in_specs=in_specs, out_specs=out_specs, check_vma=False,
    )
```

```python
import functools
import math

import jax
import jax.numpy as jnp
import ml_dtypes
import numpy as np
from jax import lax
from jax.experimental import pallas as pl
from jax.experimental.pallas import tpu as pltpu
from jax.sharding import PartitionSpec as P

BR = 4
TILE_PIX = 128
F32, BF16 = jnp.float32, jnp.bfloat16


def filter_operator(columns):
    index = np.arange(columns)
    radians = (index[:, None] * index[None, :] % columns).astype(np.float64) * (2.0 * math.pi / columns)
    table = np.concatenate([np.cos(radians), np.sin(radians)], axis=1)
    table = table.astype(np.float32).astype(ml_dtypes.bfloat16).astype(np.float64)
    frequency = np.minimum(index, columns - index) * (2.0 / (columns * columns))
    ramp = np.concatenate([frequency, frequency])
    return ((table * ramp) @ table.T).astype(np.float32).astype(ml_dtypes.bfloat16)


def kernel(
    n_gz, n_ang,
    slab_hbm, offset_hbm, view_hbm, fan_hbm, rebin_hbm, filter_hbm, tiles_hbm,
    out_ref,
    fan_v, rebin_v, filter_v, tiles_v, par_v, filt_v, place_v,
    send1, recv1, send2, recv2, slab_ref, offset_ref, view_ref,
    in_sem, tile_sem, s1, r1, s2, r2,
):
    gz, ang = lax.axis_index("gz"), lax.axis_index("ang")
    blocks, views, rows, cols = n_ang, fan_v.shape[1], fan_v.shape[0], fan_v.shape[2]
    zd = 2 * n_ang
    total_z = n_gz * zd

    def ang_at(dx, dy, dc):
        x, y, c = ang // 4, lax.rem(ang // 2, 2), lax.rem(ang, 2)
        return lax.rem(x + dx, 4) * 4 + lax.rem(y + dy, 2) * 2 + lax.rem(c + dc, 2)

    def gz_at(dy, dz):
        length = n_gz // 2
        y, z = gz // length, lax.rem(gz, length)
        return lax.rem(y + dy, 2) * length + lax.rem(z + dz, length)

    ang_order = [
        ang_at(dx, dy, dc)
        for dx, dy in ((2, 1), (1, 1), (3, 1), (2, 0), (0, 1), (1, 0), (3, 0), (0, 0))
        for dc in (1, 0)
    ]
    length = n_gz // 2
    gz_order = sorted(
        [(dy, dz) for dy in range(2) for dz in range(length)],
        key=lambda at: -at[0] - min(at[1], length - at[1]),
    )

    def ang_peer(d):
        return lax.rem(ang + d, n_ang)

    def gz_peer(d):
        return lax.rem(gz + d, n_gz)

    loads = [
        pltpu.make_async_copy(fan_hbm.at[0], fan_v, in_sem.at[0]),
        pltpu.make_async_copy(rebin_hbm, rebin_v, in_sem.at[1]),
        pltpu.make_async_copy(filter_hbm, filter_v, in_sem.at[2]),
        pltpu.make_async_copy(slab_hbm, slab_ref, in_sem.at[3]),
        pltpu.make_async_copy(offset_hbm, offset_ref, in_sem.at[4]),
        pltpu.make_async_copy(view_hbm, view_ref, in_sem.at[5]),
    ]
    for load in loads:
        load.start()

    def tile_load(i):
        return pltpu.make_async_copy(
            tiles_hbm.at[pl.ds(ang_order[i] * views, views)],
            tiles_v.at[pl.ds(i * views, views)],
            tile_sem.at[i],
        )

    for i in range(blocks):
        tile_load(i).start()

    barrier = pltpu.get_barrier_semaphore()
    for d in range(1, n_ang):
        pl.semaphore_signal(barrier, inc=1, device_id={"ang": ang_peer(d)}, device_id_type=pl.DeviceIdType.MESH)
    for d in range(1, n_gz):
        pl.semaphore_signal(barrier, inc=1, device_id={"gz": gz_peer(d)}, device_id_type=pl.DeviceIdType.MESH)

    for load in loads[3:]:
        load.wait()
    lane = lax.broadcasted_iota(jnp.int32, (1, 2 * rows), 1)
    lane = lax.rem(lane, rows)
    depth = jnp.full((1, 2 * rows), -1, jnp.int32)
    for b in range(rows // BR):
        first = slab_ref[0, b] * zd + offset_ref[0, b] - zd // 2
        depth = jnp.where(lane // BR == b, first + lax.rem(lane, BR), depth)
    slices = lax.broadcasted_iota(jnp.int32, (total_z, 2 * rows), 0)
    place_v[...] = jnp.where(slices == depth, 1.0, 0.0).astype(BF16)

    loads[0].wait()
    loads[1].wait()
    par = jnp.dot(fan_v[...].reshape(rows * views, cols), rebin_v[...], preferred_element_type=F32)
    for c in range(cols // 128):
        par_v[c * rows * views : (c + 1) * rows * views] = par[:, c * 128 : (c + 1) * 128]
    loads[2].wait()
    by_view = jnp.concatenate(
        [
            jnp.concatenate(
                [par_v[pl.ds(c * rows * views + v, rows, stride=views)].astype(BF16) for c in range(cols // 128)],
                axis=1,
            )
            for v in range(views)
        ],
        axis=0,
    )
    filtered = jnp.dot(by_view, filter_v[...], preferred_element_type=F32).astype(BF16)
    filt_v[...] = filtered.reshape(views, rows, cols)

    def send_partial(i):
        return pltpu.make_async_remote_copy(
            src_ref=send1.at[i], dst_ref=recv1.at[ang], send_sem=s1.at[i], recv_sem=r1.at[ang],
            device_id={"ang": ang_order[i]}, device_id_type=pl.DeviceIdType.MESH,
        )

    for k in range(blocks // 2):
        a, b = 2 * k, 2 * k + 1
        tile_load(a).wait()
        tile_load(b).wait()
        acc = jnp.zeros((2 * rows, 2 * TILE_PIX), F32)
        for j in range(0, views, 2):
            lhs = jnp.concatenate(
                [
                    jnp.concatenate(
                        [filt_v[view_ref[ang_order[x] * views + j + h]] for h in range(2)], axis=1
                    )
                    for x in (a, b)
                ],
                axis=0,
            )
            rhs = jnp.concatenate(
                [
                    jnp.concatenate([tiles_v[x * views + j + h] for h in range(2)], axis=0)
                    for x in (a, b)
                ],
                axis=1,
            )
            acc = acc + jnp.dot(lhs, rhs, preferred_element_type=F32)
        send1[a] = acc[:rows, :TILE_PIX].astype(BF16)
        send1[b] = acc[rows:, TILE_PIX:].astype(BF16)
        if k == 0:
            pl.semaphore_wait(barrier, n_ang + n_gz - 2)
        send_partial(a).start()
        if b < blocks - 1:
            send_partial(b).start()

    total = acc[rows:, TILE_PIX:]
    for i in range(blocks - 1):
        peer = ang_order[i]
        pltpu.make_async_remote_copy(
            src_ref=send1.at[0], dst_ref=recv1.at[peer], send_sem=s1.at[i], recv_sem=r1.at[peer],
            device_id={"ang": peer}, device_id_type=pl.DeviceIdType.MESH,
        ).wait_recv()
        total = total + recv1[peer].astype(F32)
    high = total.astype(BF16)
    low = (total - high.astype(F32)).astype(BF16)
    placed = jnp.dot(place_v[...], jnp.concatenate([high, low], axis=0), preferred_element_type=F32)
    send2[...] = placed.astype(BF16).reshape(n_gz * n_ang, 2, TILE_PIX)

    me = gz * n_ang + ang

    def send_slices(to_gz, to_ang):
        return pltpu.make_async_remote_copy(
            src_ref=send2.at[to_gz * n_ang + to_ang], dst_ref=recv2.at[me], send_sem=s2.at[0], recv_sem=r2.at[0],
            device_id={"gz": to_gz, "ang": to_ang}, device_id_type=pl.DeviceIdType.MESH,
        )

    for at in gz_order:
        to_gz = gz_at(*at)

        def send_one(d, carry, to_gz=to_gz):
            send_slices(to_gz, lax.rem(ang + d + n_ang // 2, n_ang)).start()
            return carry

        if at == (0, 0):
            lax.fori_loop(0, n_ang // 2, send_one, 0)
            lax.fori_loop(n_ang // 2 + 1, n_ang, send_one, 0)
        else:
            lax.fori_loop(0, n_ang, send_one, 0)

    recv2[me] = send2[me]
    peers = n_gz * n_ang - 1
    everything = pltpu.make_async_remote_copy(
        src_ref=send2.at[pl.ds(0, peers)], dst_ref=recv2.at[pl.ds(0, peers)], send_sem=s2.at[0], recv_sem=r2.at[0],
        device_id={"gz": gz_peer(1)}, device_id_type=pl.DeviceIdType.MESH,
    )
    everything.wait_recv()
    summed = jnp.sum(recv2[...].astype(F32).reshape(n_gz, n_ang, 2, TILE_PIX), axis=0)
    for p in range(blocks):
        out_ref[:, p * TILE_PIX : (p + 1) * TILE_PIX] = summed[p]

    for i in range(blocks - 1):
        send_partial(i).wait_send()
    everything.wait_send()


def on_device(n_gz, n_ang, fan_views, rebin_weight, slab_table, slice_offset, tiles, tile_view):
    _, rows, views, cols = fan_views.shape
    zd = 2 * n_ang
    operator = jnp.asarray(filter_operator(cols))
    dma = pltpu.SemaphoreType.DMA
    hbm = pl.BlockSpec(memory_space=pl.ANY)
    return pl.pallas_call(
        functools.partial(kernel, n_gz, n_ang),
        out_shape=jax.ShapeDtypeStruct((2, n_ang * TILE_PIX), F32),
        in_specs=[hbm] * 7,
        out_specs=pl.BlockSpec(memory_space=pltpu.VMEM),
        scratch_shapes=[
            pltpu.VMEM((rows, views, cols), BF16),
            pltpu.VMEM((cols, cols), BF16),
            pltpu.VMEM((cols, cols), BF16),
            pltpu.VMEM((n_ang * views, cols, TILE_PIX), BF16),
            pltpu.VMEM((cols // 128 * rows * views, 128), F32),
            pltpu.VMEM((views, rows, cols), BF16),
            pltpu.VMEM((n_gz * zd, 2 * rows), BF16),
            pltpu.VMEM((n_ang, rows, TILE_PIX), BF16),
            pltpu.VMEM((n_ang, rows, TILE_PIX), BF16),
            pltpu.VMEM((n_gz * n_ang, 2, TILE_PIX), BF16),
            pltpu.VMEM((n_gz * n_ang, 2, TILE_PIX), BF16),
            pltpu.SMEM((1, rows // BR), jnp.int32),
            pltpu.SMEM((1, rows // BR), jnp.int32),
            pltpu.SMEM((n_ang * views,), jnp.int32),
            dma((6,)),
            dma((n_ang,)),
            dma((n_ang,)), dma((n_ang,)),
            dma((1,)), dma((1,)),
        ],
        compiler_params=pltpu.CompilerParams(
            collective_id=0, has_side_effects=True, vmem_limit_bytes=60 * 1024 * 1024
        ),
        name="reconstruct",
    )(slab_table[:, :, 0], slice_offset, tile_view, fan_views, rebin_weight, operator, tiles)


def solution(mesh):
    n_gz, n_ang = mesh.shape["gz"], mesh.shape["ang"]
    in_specs = (
        P("gz", None, "ang", None),
        P(),
        P("gz", None, None),
        P("gz", None),
        P("ang", None, None),
        P("ang"),
    )
    out_specs = P(("gz", "ang"), None)
    return jax.shard_map(
        functools.partial(on_device, n_gz, n_ang),
        mesh=mesh, in_specs=in_specs, out_specs=out_specs, check_vma=False,
    )
```

```python
import functools
import math

import jax
import jax.numpy as jnp
import ml_dtypes
import numpy as np
from jax import lax
from jax.experimental import pallas as pl
from jax.experimental.pallas import tpu as pltpu
from jax.sharding import PartitionSpec as P

BR = 4
TILE_PIX = 128
F32, BF16 = jnp.float32, jnp.bfloat16


def filter_operator(columns):
    index = np.arange(columns)
    radians = (index[:, None] * index[None, :] % columns).astype(np.float64) * (2.0 * math.pi / columns)
    table = np.concatenate([np.cos(radians), np.sin(radians)], axis=1)
    table = table.astype(np.float32).astype(ml_dtypes.bfloat16).astype(np.float64)
    frequency = np.minimum(index, columns - index) * (2.0 / (columns * columns))
    ramp = np.concatenate([frequency, frequency])
    return ((table * ramp) @ table.T).astype(np.float32).astype(ml_dtypes.bfloat16)


def kernel(
    n_gz, n_ang,
    slab_hbm, offset_hbm, view_hbm, fan_hbm, rebin_hbm, filter_hbm, tiles_hbm,
    out_ref,
    fan_v, rebin_v, filter_v, tiles_v, par_v, filt_v, place_v,
    send0, recv0, kept, send1, recv1, send2, recv2, send3, recv3, slab_ref, offset_ref, view_ref,
    in_sem, tile_sem, s0, r0, s1, r1, s2, r2, s3, r3,
):
    gz, ang = lax.axis_index("gz"), lax.axis_index("ang")
    blocks, views, rows, cols = n_ang, fan_v.shape[1], fan_v.shape[0], fan_v.shape[2]
    zd = 2 * n_ang
    total_z = n_gz * zd

    def ang_at(dx, dy, dc):
        x, y, c = ang // 4, lax.rem(ang // 2, 2), lax.rem(ang, 2)
        return lax.rem(x + dx, 4) * 4 + lax.rem(y + dy, 2) * 2 + lax.rem(c + dc, 2)

    def gz_at(dy, dz):
        length = n_gz // 2
        y, z = gz // length, lax.rem(gz, length)
        return lax.rem(y + dy, 2) * length + lax.rem(z + dz, length)

    chips = [(2, 1), (1, 1), (3, 1), (0, 1), (2, 0), (1, 0), (3, 0), (0, 0)]
    ang_order = [ang_at(dx, dy, dc) for dx, dy in chips for dc in (1, 0)]
    length = n_gz // 2
    gz_order = sorted(
        [(dy, dz) for dy in range(2) for dz in range(length)],
        key=lambda at: -at[0] - min(at[1], length - at[1]),
    )

    gz_order = [gz_at(*at) for at in gz_order]

    loads = [
        pltpu.make_async_copy(fan_hbm.at[0], fan_v, in_sem.at[0]),
        pltpu.make_async_copy(rebin_hbm, rebin_v, in_sem.at[1]),
        pltpu.make_async_copy(filter_hbm, filter_v, in_sem.at[2]),
        pltpu.make_async_copy(slab_hbm, slab_ref, in_sem.at[3]),
        pltpu.make_async_copy(offset_hbm, offset_ref, in_sem.at[4]),
        pltpu.make_async_copy(view_hbm, view_ref, in_sem.at[5]),
    ]
    for load in loads:
        load.start()

    def tile_load(i):
        return pltpu.make_async_copy(
            tiles_hbm.at[pl.ds(ang_order[i] * views, views)],
            tiles_v.at[pl.ds(i * views, views)],
            tile_sem.at[i],
        )

    for i in range(blocks):
        tile_load(i).start()

    barrier = pltpu.get_barrier_semaphore()
    for peer in gz_order[:-1]:
        pl.semaphore_signal(barrier, inc=1, device_id={"gz": peer}, device_id_type=pl.DeviceIdType.MESH)
    for peer in ang_order[:-1]:
        pl.semaphore_signal(barrier, inc=1, device_id={"ang": peer}, device_id_type=pl.DeviceIdType.MESH)

    for load in loads[3:]:
        load.wait()
    lane = lax.broadcasted_iota(jnp.int32, (1, 2 * rows), 1)
    lane = lax.rem(lane, rows)
    depth = jnp.full((1, 2 * rows), -1, jnp.int32)
    for b in range(rows // BR):
        first = slab_ref[0, b] * zd + offset_ref[0, b] - zd // 2
        depth = jnp.where(lane // BR == b, first + lax.rem(lane, BR), depth)
    slices = lax.broadcasted_iota(jnp.int32, (total_z, 2 * rows), 0)
    place_v[...] = jnp.where(slices == depth, 1.0, 0.0).astype(BF16)

    loads[0].wait()
    loads[1].wait()
    par = jnp.dot(fan_v[...].reshape(rows * views, cols), rebin_v[...], preferred_element_type=F32)
    for c in range(cols // 128):
        par_v[c * rows * views : (c + 1) * rows * views] = par[:, c * 128 : (c + 1) * 128]
    loads[2].wait()
    by_view = jnp.concatenate(
        [
            jnp.concatenate(
                [par_v[pl.ds(c * rows * views + v, rows, stride=views)].astype(BF16) for c in range(cols // 128)],
                axis=1,
            )
            for v in range(views)
        ],
        axis=0,
    )
    filtered = jnp.dot(by_view, filter_v[...], preferred_element_type=F32).astype(BF16)
    filt_v[...] = filtered.reshape(views, rows, cols)

    def send_sibling(k):
        return pltpu.make_async_remote_copy(
            src_ref=send0.at[k], dst_ref=recv0.at[k], send_sem=s0.at[k], recv_sem=r0.at[k],
            device_id={"ang": ang_at(0, 0, 1)}, device_id_type=pl.DeviceIdType.MESH,
        )

    def send_partial(k):
        return pltpu.make_async_remote_copy(
            src_ref=send1.at[k], dst_ref=recv1.at[ang // 2], send_sem=s1.at[k], recv_sem=r1.at[ang // 2],
            device_id={"ang": ang_order[2 * k + 1]}, device_id_type=pl.DeviceIdType.MESH,
        )

    def chip_sum(k):
        send_sibling(k).wait_recv()
        return kept[k] + recv0[k]

    last = blocks // 2 - 1
    for k in range(blocks // 2):
        a, b = 2 * k, 2 * k + 1
        tile_load(a).wait()
        tile_load(b).wait()
        acc = jnp.zeros((2 * rows, 2 * TILE_PIX), F32)
        for j in range(0, views, 2):
            lhs = jnp.concatenate(
                [
                    jnp.concatenate(
                        [filt_v[view_ref[ang_order[x] * views + j + h]] for h in range(2)], axis=1
                    )
                    for x in (a, b)
                ],
                axis=0,
            )
            rhs = jnp.concatenate(
                [
                    jnp.concatenate([tiles_v[x * views + j + h] for h in range(2)], axis=0)
                    for x in (a, b)
                ],
                axis=1,
            )
            acc = acc + jnp.dot(lhs, rhs, preferred_element_type=F32)
        send0[k] = acc[:rows, :TILE_PIX]
        kept[k] = acc[rows:, TILE_PIX:]
        if k == 0:
            pl.semaphore_wait(barrier, n_ang + n_gz - 2)
        send_sibling(k).start()
        if k > 0:
            send1[k - 1] = chip_sum(k - 1).astype(BF16)
            send_partial(k - 1).start()

    def wait_recv(buffer, sem, index):
        pltpu.make_async_remote_copy(
            src_ref=buffer.at[index], dst_ref=buffer.at[index], send_sem=sem.at[index], recv_sem=sem.at[index],
            device_id={"ang": ang_at(0, 0, 1)}, device_id_type=pl.DeviceIdType.MESH,
        ).wait_recv()

    total = chip_sum(last)
    for k in range(last):
        chip = ang_order[2 * k + 1] // 2
        wait_recv(recv1, r1, chip)
        total = total + recv1[chip].astype(F32)
    high = total.astype(BF16)
    low = (total - high.astype(F32)).astype(BF16)
    placed = jnp.dot(place_v[...], jnp.concatenate([high, low], axis=0), preferred_element_type=F32)
    send2[...] = placed.astype(BF16).reshape(n_gz, zd, TILE_PIX)

    def send_slab(to):
        return pltpu.make_async_remote_copy(
            src_ref=send2.at[to], dst_ref=recv2.at[gz], send_sem=s2.at[to], recv_sem=r2.at[gz],
            device_id={"gz": to}, device_id_type=pl.DeviceIdType.MESH,
        )

    for to in gz_order[:-1]:
        send_slab(to).start()
    slab = send2[gz].astype(F32)
    for peer in reversed(gz_order[:-1]):
        wait_recv(recv2, r2, peer)
        slab = slab + recv2[peer].astype(F32)

    send3[...] = slab.reshape(n_ang, 2, TILE_PIX)

    def send_slices(to):
        return pltpu.make_async_remote_copy(
            src_ref=send3.at[to], dst_ref=recv3.at[ang], send_sem=s3.at[to], recv_sem=r3.at[ang],
            device_id={"ang": to}, device_id_type=pl.DeviceIdType.MESH,
        )

    for to in ang_order[:-1]:
        send_slices(to).start()
    recv3[ang] = send3[ang]
    for k in range(last + 1):
        send_sibling(k).wait_send()
    for k in range(last):
        send_partial(k).wait_send()
    for to in gz_order[:-1]:
        send_slab(to).wait_send()
    for peer in reversed(ang_order[:-1]):
        wait_recv(recv3, r3, peer)
    for p in range(blocks):
        out_ref[:, p * TILE_PIX : (p + 1) * TILE_PIX] = recv3[p]
    for to in ang_order[:-1]:
        send_slices(to).wait_send()


def on_device(n_gz, n_ang, fan_views, rebin_weight, slab_table, slice_offset, tiles, tile_view):
    _, rows, views, cols = fan_views.shape
    zd = 2 * n_ang
    operator = jnp.asarray(filter_operator(cols))
    dma = pltpu.SemaphoreType.DMA
    hbm = pl.BlockSpec(memory_space=pl.ANY)
    return pl.pallas_call(
        functools.partial(kernel, n_gz, n_ang),
        out_shape=jax.ShapeDtypeStruct((2, n_ang * TILE_PIX), F32),
        in_specs=[hbm] * 7,
        out_specs=pl.BlockSpec(memory_space=pltpu.VMEM),
        scratch_shapes=[
            pltpu.VMEM((rows, views, cols), BF16),
            pltpu.VMEM((cols, cols), BF16),
            pltpu.VMEM((cols, cols), BF16),
            pltpu.VMEM((n_ang * views, cols, TILE_PIX), BF16),
            pltpu.VMEM((cols // 128 * rows * views, 128), F32),
            pltpu.VMEM((views, rows, cols), BF16),
            pltpu.VMEM((n_gz * zd, 2 * rows), BF16),
            pltpu.VMEM((n_ang // 2, rows, TILE_PIX), F32),
            pltpu.VMEM((n_ang // 2, rows, TILE_PIX), F32),
            pltpu.VMEM((n_ang // 2, rows, TILE_PIX), F32),
            pltpu.VMEM((n_ang // 2, rows, TILE_PIX), BF16),
            pltpu.VMEM((n_ang // 2, rows, TILE_PIX), BF16),
            pltpu.VMEM((n_gz, zd, TILE_PIX), BF16),
            pltpu.VMEM((n_gz, zd, TILE_PIX), BF16),
            pltpu.VMEM((n_ang, 2, TILE_PIX), F32),
            pltpu.VMEM((n_ang, 2, TILE_PIX), F32),
            pltpu.SMEM((1, rows // BR), jnp.int32),
            pltpu.SMEM((1, rows // BR), jnp.int32),
            pltpu.SMEM((n_ang * views,), jnp.int32),
            dma((6,)),
            dma((n_ang,)),
            dma((n_ang // 2,)), dma((n_ang // 2,)),
            dma((n_ang // 2,)), dma((n_ang // 2,)),
            dma((n_gz,)), dma((n_gz,)),
            dma((n_ang,)), dma((n_ang,)),
        ],
        compiler_params=pltpu.CompilerParams(
            collective_id=0, has_side_effects=True, vmem_limit_bytes=60 * 1024 * 1024
        ),
        name="reconstruct",
    )(slab_table[:, :, 0], slice_offset, tile_view, fan_views, rebin_weight, operator, tiles)


def solution(mesh):
    n_gz, n_ang = mesh.shape["gz"], mesh.shape["ang"]
    in_specs = (
        P("gz", None, "ang", None),
        P(),
        P("gz", None, None),
        P("gz", None),
        P("ang", None, None),
        P("ang"),
    )
    out_specs = P(("gz", "ang"), None)
    return jax.shard_map(
        functools.partial(on_device, n_gz, n_ang),
        mesh=mesh, in_specs=in_specs, out_specs=out_specs, check_vma=False,
    )
```

```python
import functools
import math

import jax
import jax.numpy as jnp
import ml_dtypes
import numpy as np
from jax import lax
from jax.experimental import pallas as pl
from jax.experimental.pallas import tpu as pltpu
from jax.sharding import PartitionSpec as P

BR = 4
TILE_PIX = 128
F32, BF16 = jnp.float32, jnp.bfloat16


def filter_operator(columns):
    index = np.arange(columns)
    radians = (index[:, None] * index[None, :] % columns).astype(np.float64) * (2.0 * math.pi / columns)
    table = np.concatenate([np.cos(radians), np.sin(radians)], axis=1)
    table = table.astype(np.float32).astype(ml_dtypes.bfloat16).astype(np.float64)
    frequency = np.minimum(index, columns - index) * (2.0 / (columns * columns))
    ramp = np.concatenate([frequency, frequency])
    return ((table * ramp) @ table.T).astype(np.float32).astype(ml_dtypes.bfloat16)


def kernel(
    n_gz, n_ang,
    slab_hbm, offset_hbm, view_hbm, fan_hbm, rebin_hbm, filter_hbm, tiles_hbm,
    out_ref,
    fan_v, rebin_v, filter_v, tiles_v, par_v, filt_v, place_v,
    send0, recv0, kept, send1, recv1, send2, recv2, send3, recv3, slab_ref, offset_ref, view_ref,
    in_sem, tile_sem, s0, r0, s1, r1, s2, r2, s3, r3,
):
    gz, ang = lax.axis_index("gz"), lax.axis_index("ang")
    blocks, views, rows, cols = n_ang, fan_v.shape[1], fan_v.shape[0], fan_v.shape[2]
    zd = 2 * n_ang
    total_z = n_gz * zd

    def ang_at(dx, dy, dc):
        x, y, c = ang // 4, lax.rem(ang // 2, 2), lax.rem(ang, 2)
        return lax.rem(x + dx, 4) * 4 + lax.rem(y + dy, 2) * 2 + lax.rem(c + dc, 2)

    def owner(i):
        k = i // 2
        return ang_at(lax.rem(k + 1, 4), 1 - k // 4, 1 - lax.rem(i, 2))

    def gz_at(dy, dz):
        length = n_gz // 2
        y, z = gz // length, lax.rem(gz, length)
        return lax.rem(y + dy, 2) * length + lax.rem(z + dz, length)

    ang_order = [owner(jnp.int32(i)) for i in range(n_ang)]
    length = n_gz // 2
    gz_order = sorted(
        [(dy, dz) for dy in range(2) for dz in range(length)],
        key=lambda at: -at[0] - min(at[1], length - at[1]),
    )

    gz_order = [gz_at(*at) for at in gz_order]

    loads = [
        pltpu.make_async_copy(fan_hbm.at[0], fan_v, in_sem.at[0]),
        pltpu.make_async_copy(rebin_hbm, rebin_v, in_sem.at[1]),
        pltpu.make_async_copy(filter_hbm, filter_v, in_sem.at[2]),
        pltpu.make_async_copy(slab_hbm, slab_ref, in_sem.at[3]),
        pltpu.make_async_copy(offset_hbm, offset_ref, in_sem.at[4]),
        pltpu.make_async_copy(view_hbm, view_ref, in_sem.at[5]),
    ]
    for load in loads:
        load.start()

    def tile_load(i):
        return pltpu.make_async_copy(
            tiles_hbm.at[pl.ds(owner(i) * views, views)],
            tiles_v.at[pl.ds(i * views, views)],
            tile_sem.at[i],
        )

    def start_tile(i, carry):
        tile_load(i).start()
        return carry

    lax.fori_loop(0, blocks, start_tile, 0)

    barrier = pltpu.get_barrier_semaphore()
    for peer in gz_order[:-1]:
        pl.semaphore_signal(barrier, inc=1, device_id={"gz": peer}, device_id_type=pl.DeviceIdType.MESH)
    for peer in ang_order[:-1]:
        pl.semaphore_signal(barrier, inc=1, device_id={"ang": peer}, device_id_type=pl.DeviceIdType.MESH)

    for load in loads[3:]:
        load.wait()
    lane = lax.broadcasted_iota(jnp.int32, (1, 2 * rows), 1)
    lane = lax.rem(lane, rows)
    depth = jnp.full((1, 2 * rows), -1, jnp.int32)
    for b in range(rows // BR):
        first = slab_ref[0, b] * zd + offset_ref[0, b] - zd // 2
        depth = jnp.where(lane // BR == b, first + lax.rem(lane, BR), depth)
    slices = lax.broadcasted_iota(jnp.int32, (total_z, 2 * rows), 0)
    place_v[...] = jnp.where(slices == depth, 1.0, 0.0).astype(BF16)

    loads[0].wait()
    loads[1].wait()
    step = 16

    def rebin(r, carry):
        part = fan_v[pl.ds(r * step, step)].reshape(step * views, cols)
        par = jnp.dot(part, rebin_v[...], preferred_element_type=F32)
        for c in range(cols // 128):
            start = c * rows * views + r * (step * views)
            par_v[pl.ds(pl.multiple_of(start, 8), step * views)] = par[:, c * 128 : (c + 1) * 128]
        return carry

    lax.fori_loop(0, rows // step, rebin, 0)
    loads[2].wait()

    def ramp(w, carry):
        by_view = jnp.concatenate(
            [
                jnp.concatenate(
                    [
                        par_v[pl.ds(c * rows * views + 2 * w + h, rows, stride=views)].astype(BF16)
                        for c in range(cols // 128)
                    ],
                    axis=1,
                )
                for h in range(2)
            ],
            axis=0,
        )
        filtered = jnp.dot(by_view, filter_v[...], preferred_element_type=F32).astype(BF16)
        filt_v[pl.ds(2 * w, 2)] = filtered.reshape(2, rows, cols)
        return carry

    lax.fori_loop(0, views // 2, ramp, 0)

    def send_sibling(k):
        return pltpu.make_async_remote_copy(
            src_ref=send0.at[k], dst_ref=recv0.at[k], send_sem=s0.at[k], recv_sem=r0.at[k],
            device_id={"ang": ang_at(0, 0, 1)}, device_id_type=pl.DeviceIdType.MESH,
        )

    def send_partial(k):
        return pltpu.make_async_remote_copy(
            src_ref=send1.at[k], dst_ref=recv1.at[ang // 2], send_sem=s1.at[k], recv_sem=r1.at[ang // 2],
            device_id={"ang": owner(2 * k + 1)}, device_id_type=pl.DeviceIdType.MESH,
        )

    def chip_sum(k):
        send_sibling(k).wait_recv()
        return kept[k] + recv0[k]

    last = blocks // 2 - 1
    pl.semaphore_wait(barrier, n_ang + n_gz - 2)

    def pair(k, carry):
        a, b = 2 * k, 2 * k + 1
        tile_load(a).wait()
        tile_load(b).wait()
        acc = jnp.zeros((2 * rows, 2 * TILE_PIX), F32)
        for j in range(0, views, 2):
            lhs = jnp.concatenate(
                [
                    jnp.concatenate([filt_v[view_ref[owner(x) * views + j + h]] for h in range(2)], axis=1)
                    for x in (a, b)
                ],
                axis=0,
            )
            rhs = jnp.concatenate(
                [
                    jnp.concatenate([tiles_v[x * views + j + h] for h in range(2)], axis=0)
                    for x in (a, b)
                ],
                axis=1,
            )
            acc = acc + jnp.dot(lhs, rhs, preferred_element_type=F32)
        send0[k] = acc[:rows, :TILE_PIX]
        kept[k] = acc[rows:, TILE_PIX:]
        send_sibling(k).start()

        @pl.when(k > 0)
        def _():
            send1[k - 1] = chip_sum(k - 1).astype(BF16)
            send_partial(k - 1).start()

        return carry

    lax.fori_loop(0, blocks // 2, pair, 0)

    def wait_recv(buffer, sem, index):
        pltpu.make_async_remote_copy(
            src_ref=buffer.at[index], dst_ref=buffer.at[index], send_sem=sem.at[index], recv_sem=sem.at[index],
            device_id={"ang": ang_at(0, 0, 1)}, device_id_type=pl.DeviceIdType.MESH,
        ).wait_recv()

    total = chip_sum(last)
    for k in range(last):
        chip = ang_order[2 * k + 1] // 2
        wait_recv(recv1, r1, chip)
        total = total + recv1[chip].astype(F32)
    high = total.astype(BF16)
    low = (total - high.astype(F32)).astype(BF16)
    placed = jnp.dot(place_v[...], jnp.concatenate([high, low], axis=0), preferred_element_type=F32)
    send2[...] = placed.astype(BF16).reshape(n_gz, zd, TILE_PIX)

    def send_slab(to):
        return pltpu.make_async_remote_copy(
            src_ref=send2.at[to], dst_ref=recv2.at[gz], send_sem=s2.at[to], recv_sem=r2.at[gz],
            device_id={"gz": to}, device_id_type=pl.DeviceIdType.MESH,
        )

    for to in gz_order[:-1]:
        send_slab(to).start()
    slab = send2[gz].astype(F32)
    for peer in reversed(gz_order[:-1]):
        wait_recv(recv2, r2, peer)
        slab = slab + recv2[peer].astype(F32)

    send3[...] = slab.reshape(n_ang, 2, TILE_PIX)

    def send_slices(to):
        return pltpu.make_async_remote_copy(
            src_ref=send3.at[to], dst_ref=recv3.at[ang], send_sem=s3.at[to], recv_sem=r3.at[ang],
            device_id={"ang": to}, device_id_type=pl.DeviceIdType.MESH,
        )

    for to in ang_order[:-1]:
        send_slices(to).start()
    recv3[ang] = send3[ang]
    for k in range(last + 1):
        send_sibling(k).wait_send()
    for k in range(last):
        send_partial(k).wait_send()
    for to in gz_order[:-1]:
        send_slab(to).wait_send()
    for peer in reversed(ang_order[:-1]):
        wait_recv(recv3, r3, peer)
    for p in range(blocks):
        out_ref[:, p * TILE_PIX : (p + 1) * TILE_PIX] = recv3[p]
    for to in ang_order[:-1]:
        send_slices(to).wait_send()


def on_device(n_gz, n_ang, fan_views, rebin_weight, slab_table, slice_offset, tiles, tile_view):
    _, rows, views, cols = fan_views.shape
    zd = 2 * n_ang
    operator = jnp.asarray(filter_operator(cols))
    dma = pltpu.SemaphoreType.DMA
    hbm = pl.BlockSpec(memory_space=pl.ANY)
    return pl.pallas_call(
        functools.partial(kernel, n_gz, n_ang),
        out_shape=jax.ShapeDtypeStruct((2, n_ang * TILE_PIX), F32),
        in_specs=[hbm] * 7,
        out_specs=pl.BlockSpec(memory_space=pltpu.VMEM),
        scratch_shapes=[
            pltpu.VMEM((rows, views, cols), BF16),
            pltpu.VMEM((cols, cols), BF16),
            pltpu.VMEM((cols, cols), BF16),
            pltpu.VMEM((n_ang * views, cols, TILE_PIX), BF16),
            pltpu.VMEM((cols // 128 * rows * views, 128), F32),
            pltpu.VMEM((views, rows, cols), BF16),
            pltpu.VMEM((n_gz * zd, 2 * rows), BF16),
            pltpu.VMEM((n_ang // 2, rows, TILE_PIX), F32),
            pltpu.VMEM((n_ang // 2, rows, TILE_PIX), F32),
            pltpu.VMEM((n_ang // 2, rows, TILE_PIX), F32),
            pltpu.VMEM((n_ang // 2, rows, TILE_PIX), BF16),
            pltpu.VMEM((n_ang // 2, rows, TILE_PIX), BF16),
            pltpu.VMEM((n_gz, zd, TILE_PIX), BF16),
            pltpu.VMEM((n_gz, zd, TILE_PIX), BF16),
            pltpu.VMEM((n_ang, 2, TILE_PIX), F32),
            pltpu.VMEM((n_ang, 2, TILE_PIX), F32),
            pltpu.SMEM((1, rows // BR), jnp.int32),
            pltpu.SMEM((1, rows // BR), jnp.int32),
            pltpu.SMEM((n_ang * views,), jnp.int32),
            dma((6,)),
            dma((n_ang,)),
            dma((n_ang // 2,)), dma((n_ang // 2,)),
            dma((n_ang // 2,)), dma((n_ang // 2,)),
            dma((n_gz,)), dma((n_gz,)),
            dma((n_ang,)), dma((n_ang,)),
        ],
        compiler_params=pltpu.CompilerParams(
            collective_id=0, has_side_effects=True, vmem_limit_bytes=60 * 1024 * 1024
        ),
        name="reconstruct",
    )(slab_table[:, :, 0], slice_offset, tile_view, fan_views, rebin_weight, operator, tiles)


def solution(mesh):
    n_gz, n_ang = mesh.shape["gz"], mesh.shape["ang"]
    in_specs = (
        P("gz", None, "ang", None),
        P(),
        P("gz", None, None),
        P("gz", None),
        P("ang", None, None),
        P("ang"),
    )
    out_specs = P(("gz", "ang"), None)
    return jax.shard_map(
        functools.partial(on_device, n_gz, n_ang),
        mesh=mesh, in_specs=in_specs, out_specs=out_specs, check_vma=False,
    )
```

```python
import functools
import math

import jax
import jax.numpy as jnp
import ml_dtypes
import numpy as np
from jax import lax
from jax.experimental import pallas as pl
from jax.experimental.pallas import tpu as pltpu
from jax.sharding import PartitionSpec as P

BR = 4
TILE_PIX = 128
F32, BF16 = jnp.float32, jnp.bfloat16


def filter_operator(columns):
    index = np.arange(columns)
    radians = (index[:, None] * index[None, :] % columns).astype(np.float64) * (2.0 * math.pi / columns)
    table = np.concatenate([np.cos(radians), np.sin(radians)], axis=1)
    table = table.astype(np.float32).astype(ml_dtypes.bfloat16).astype(np.float64)
    frequency = np.minimum(index, columns - index) * (2.0 / (columns * columns))
    ramp = np.concatenate([frequency, frequency])
    return ((table * ramp) @ table.T).astype(np.float32).astype(ml_dtypes.bfloat16)


def kernel(
    n_gz, n_ang,
    slab_hbm, offset_hbm, view_hbm, fan_hbm, rebin_hbm, filter_hbm, tiles_hbm,
    out_ref,
    fan_v, rebin_v, filter_v, tiles_v, par_v, filt_v, place_v,
    send0, recv0, kept, direct, arrived, send1, recv1, send2, recv2, send3, recv3, slab_ref, offset_ref, view_ref,
    in_sem, tile_sem, s0, r0, sd, rd, s1, r1, s2, r2, s3, r3,
):
    gz, ang = lax.axis_index("gz"), lax.axis_index("ang")
    blocks, views, rows, cols = n_ang, fan_v.shape[1], fan_v.shape[0], fan_v.shape[2]
    zd = 2 * n_ang
    total_z = n_gz * zd

    def ang_at(dx, dy, dc):
        x, y, c = ang // 4, lax.rem(ang // 2, 2), lax.rem(ang, 2)
        return lax.rem(x + dx, 4) * 4 + lax.rem(y + dy, 2) * 2 + lax.rem(c + dc, 2)

    def owner(i):
        k = i // 2
        return ang_at(lax.rem(k + 1, 4), 1 - k // 4, 1 - lax.rem(i, 2))

    def gz_at(dy, dz):
        length = n_gz // 2
        y, z = gz // length, lax.rem(gz, length)
        return lax.rem(y + dy, 2) * length + lax.rem(z + dz, length)

    ang_order = [owner(jnp.int32(i)) for i in range(n_ang)]
    length = n_gz // 2
    gz_order = sorted(
        [(dy, dz) for dy in range(2) for dz in range(length)],
        key=lambda at: -at[0] - min(at[1], length - at[1]),
    )

    gz_order = [gz_at(*at) for at in gz_order]

    barrier = pltpu.get_barrier_semaphore()
    for peer in gz_order[:-1]:
        pl.semaphore_signal(barrier, inc=1, device_id={"gz": peer}, device_id_type=pl.DeviceIdType.MESH)
    for peer in ang_order[:-1]:
        pl.semaphore_signal(barrier, inc=1, device_id={"ang": peer}, device_id_type=pl.DeviceIdType.MESH)

    loads = [
        pltpu.make_async_copy(fan_hbm.at[0], fan_v, in_sem.at[0]),
        pltpu.make_async_copy(rebin_hbm, rebin_v, in_sem.at[1]),
        pltpu.make_async_copy(filter_hbm, filter_v, in_sem.at[2]),
        pltpu.make_async_copy(slab_hbm, slab_ref, in_sem.at[3]),
        pltpu.make_async_copy(offset_hbm, offset_ref, in_sem.at[4]),
        pltpu.make_async_copy(view_hbm, view_ref, in_sem.at[5]),
    ]
    for load in loads:
        load.start()

    def tile_load(i):
        return pltpu.make_async_copy(
            tiles_hbm.at[pl.ds(owner(i) * views, views)],
            tiles_v.at[pl.ds(i * views, views)],
            tile_sem.at[i],
        )

    def start_tile(i, carry):
        tile_load(i).start()
        return carry

    lax.fori_loop(0, blocks, start_tile, 0)

    for load in loads[3:]:
        load.wait()
    lane = lax.broadcasted_iota(jnp.int32, (1, 2 * rows), 1)
    lane = lax.rem(lane, rows)
    depth = jnp.full((1, 2 * rows), -1, jnp.int32)
    for b in range(rows // BR):
        first = slab_ref[0, b] * zd + offset_ref[0, b] - zd // 2
        depth = jnp.where(lane // BR == b, first + lax.rem(lane, BR), depth)
    slices = lax.broadcasted_iota(jnp.int32, (total_z, 2 * rows), 0)
    place_v[...] = jnp.where(slices == depth, 1.0, 0.0).astype(BF16)

    loads[0].wait()
    loads[1].wait()
    step = 16

    def rebin(r, carry):
        part = fan_v[pl.ds(r * step, step)].reshape(step * views, cols)
        par = jnp.dot(part, rebin_v[...], preferred_element_type=F32)
        for c in range(cols // 128):
            start = c * rows * views + r * (step * views)
            par_v[pl.ds(pl.multiple_of(start, 8), step * views)] = par[:, c * 128 : (c + 1) * 128]
        return carry

    lax.fori_loop(0, rows // step, rebin, 0)
    loads[2].wait()

    def ramp(w, carry):
        by_view = jnp.concatenate(
            [
                jnp.concatenate(
                    [
                        par_v[pl.ds(c * rows * views + 2 * w + h, rows, stride=views)].astype(BF16)
                        for c in range(cols // 128)
                    ],
                    axis=1,
                )
                for h in range(2)
            ],
            axis=0,
        )
        filtered = jnp.dot(by_view, filter_v[...], preferred_element_type=F32).astype(BF16)
        filt_v[pl.ds(2 * w, 2)] = filtered.reshape(2, rows, cols)
        return carry

    lax.fori_loop(0, views // 2, ramp, 0)

    last = blocks // 2 - 1

    def send_sibling(k):
        return pltpu.make_async_remote_copy(
            src_ref=send0.at[k], dst_ref=recv0.at[k], send_sem=s0.at[k], recv_sem=r0.at[k],
            device_id={"ang": ang_at(0, 0, 1)}, device_id_type=pl.DeviceIdType.MESH,
        )

    def send_partial(k):
        return pltpu.make_async_remote_copy(
            src_ref=send1.at[k], dst_ref=recv1.at[ang // 2], send_sem=s1.at[k], recv_sem=r1.at[ang // 2],
            device_id={"ang": owner(2 * k + 1)}, device_id_type=pl.DeviceIdType.MESH,
        )

    def send_direct(h):
        core = lax.rem(ang, 2)
        return pltpu.make_async_remote_copy(
            src_ref=direct.at[h], dst_ref=arrived.at[core], send_sem=sd.at[h], recv_sem=rd.at[core],
            device_id={"ang": owner(2 * (last - 1) + h)}, device_id_type=pl.DeviceIdType.MESH,
        )

    def chip_sum(k):
        send_sibling(k).wait_recv()
        return kept[k] + recv0[k]

    pl.semaphore_wait(barrier, n_ang + n_gz - 2)

    def pair(k, carry):
        a, b = 2 * k, 2 * k + 1
        tile_load(a).wait()
        tile_load(b).wait()
        acc = jnp.zeros((2 * rows, 2 * TILE_PIX), F32)
        for j in range(0, views, 2):
            lhs = jnp.concatenate(
                [
                    jnp.concatenate([filt_v[view_ref[owner(x) * views + j + h]] for h in range(2)], axis=1)
                    for x in (a, b)
                ],
                axis=0,
            )
            rhs = jnp.concatenate(
                [
                    jnp.concatenate([tiles_v[x * views + j + h] for h in range(2)], axis=0)
                    for x in (a, b)
                ],
                axis=1,
            )
            acc = acc + jnp.dot(lhs, rhs, preferred_element_type=F32)
        send0[k] = acc[:rows, :TILE_PIX]
        kept[k] = acc[rows:, TILE_PIX:]

        @pl.when(k != last - 1)
        def _():
            send_sibling(k).start()

        @pl.when(k == last - 1)
        def _():
            direct[0] = send0[k].astype(BF16)
            direct[1] = kept[k].astype(BF16)
            for h in range(2):
                send_direct(h).start()

        @pl.when((k > 0) & (k < last))
        def _():
            send1[k - 1] = chip_sum(k - 1).astype(BF16)
            send_partial(k - 1).start()

        return carry

    lax.fori_loop(0, blocks // 2, pair, 0)

    def wait_recv(buffer, sem, index):
        pltpu.make_async_remote_copy(
            src_ref=buffer.at[index], dst_ref=buffer.at[index], send_sem=sem.at[index], recv_sem=sem.at[index],
            device_id={"ang": ang_at(0, 0, 1)}, device_id_type=pl.DeviceIdType.MESH,
        ).wait_recv()

    total = chip_sum(last)
    for h in range(2):
        wait_recv(arrived, rd, h)
        total = total + arrived[h].astype(F32)
    for k in range(last - 1):
        chip = ang_at((3 - k) % 4, 1 - k // 4, 0) // 2
        wait_recv(recv1, r1, chip)
        total = total + recv1[chip].astype(F32)
    high = total.astype(BF16)
    low = (total - high.astype(F32)).astype(BF16)
    placed = jnp.dot(place_v[...], jnp.concatenate([high, low], axis=0), preferred_element_type=F32)
    send2[...] = placed.astype(BF16).reshape(n_gz, zd, TILE_PIX)

    def send_slab(to):
        return pltpu.make_async_remote_copy(
            src_ref=send2.at[to], dst_ref=recv2.at[gz], send_sem=s2.at[to], recv_sem=r2.at[gz],
            device_id={"gz": to}, device_id_type=pl.DeviceIdType.MESH,
        )

    for to in gz_order[:-1]:
        send_slab(to).start()
    halves = [send2[gz].astype(F32), jnp.zeros((zd, TILE_PIX), F32)]
    for x, peer in enumerate(reversed(gz_order[:-1])):
        wait_recv(recv2, r2, peer)
        halves[x % 2] = halves[x % 2] + recv2[peer].astype(F32)

    for h in range(2):
        send3[:, h] = halves[h].reshape(n_ang, 2, TILE_PIX)

    def send_slices(to):
        return pltpu.make_async_remote_copy(
            src_ref=send3.at[to], dst_ref=recv3.at[ang], send_sem=s3.at[to], recv_sem=r3.at[ang],
            device_id={"ang": to}, device_id_type=pl.DeviceIdType.MESH,
        )

    for to in ang_order[:-1]:
        send_slices(to).start()
    recv3[ang] = send3[ang]
    for h in range(2):
        send_direct(h).wait_send()
    for k in range(last + 1):
        if k != last - 1:
            send_sibling(k).wait_send()
    for k in range(last - 1):
        send_partial(k).wait_send()
    for to in gz_order[:-1]:
        send_slab(to).wait_send()
    for peer in reversed(ang_order[:-1]):
        wait_recv(recv3, r3, peer)
    for h in range(2):
        out_ref[h] = recv3[:, h]
    for to in ang_order[:-1]:
        send_slices(to).wait_send()


def on_device(n_gz, n_ang, fan_views, rebin_weight, slab_table, slice_offset, tiles, tile_view):
    _, rows, views, cols = fan_views.shape
    zd = 2 * n_ang
    operator = jnp.asarray(filter_operator(cols))
    dma = pltpu.SemaphoreType.DMA
    hbm = pl.BlockSpec(memory_space=pl.ANY)
    pieces = pl.pallas_call(
        functools.partial(kernel, n_gz, n_ang),
        out_shape=jax.ShapeDtypeStruct((2, n_ang, 2, TILE_PIX), F32),
        in_specs=[hbm] * 7,
        out_specs=pl.BlockSpec(memory_space=pltpu.VMEM),
        scratch_shapes=[
            pltpu.VMEM((rows, views, cols), BF16),
            pltpu.VMEM((cols, cols), BF16),
            pltpu.VMEM((cols, cols), BF16),
            pltpu.VMEM((n_ang * views, cols, TILE_PIX), BF16),
            pltpu.VMEM((cols // 128 * rows * views, 128), F32),
            pltpu.VMEM((views, rows, cols), BF16),
            pltpu.VMEM((n_gz * zd, 2 * rows), BF16),
            pltpu.VMEM((n_ang // 2, rows, TILE_PIX), F32),
            pltpu.VMEM((n_ang // 2, rows, TILE_PIX), F32),
            pltpu.VMEM((n_ang // 2, rows, TILE_PIX), F32),
            pltpu.VMEM((2, rows, TILE_PIX), BF16),
            pltpu.VMEM((2, rows, TILE_PIX), BF16),
            pltpu.VMEM((n_ang // 2, rows, TILE_PIX), BF16),
            pltpu.VMEM((n_ang // 2, rows, TILE_PIX), BF16),
            pltpu.VMEM((n_gz, zd, TILE_PIX), BF16),
            pltpu.VMEM((n_gz, zd, TILE_PIX), BF16),
            pltpu.VMEM((n_ang, 2, 2, TILE_PIX), F32),
            pltpu.VMEM((n_ang, 2, 2, TILE_PIX), F32),
            pltpu.SMEM((1, rows // BR), jnp.int32),
            pltpu.SMEM((1, rows // BR), jnp.int32),
            pltpu.SMEM((n_ang * views,), jnp.int32),
            dma((6,)),
            dma((n_ang,)),
            dma((n_ang // 2,)), dma((n_ang // 2,)),
            dma((2,)), dma((2,)),
            dma((n_ang // 2,)), dma((n_ang // 2,)),
            dma((n_gz,)), dma((n_gz,)),
            dma((n_ang,)), dma((n_ang,)),
        ],
        compiler_params=pltpu.CompilerParams(
            collective_id=0, has_side_effects=True, vmem_limit_bytes=60 * 1024 * 1024
        ),
        name="reconstruct",
    )(slab_table[:, :, 0], slice_offset, tile_view, fan_views, rebin_weight, operator, tiles)
    return (pieces[0] + pieces[1]).transpose(1, 0, 2).reshape(2, n_ang * TILE_PIX)


def solution(mesh):
    n_gz, n_ang = mesh.shape["gz"], mesh.shape["ang"]
    in_specs = (
        P("gz", None, "ang", None),
        P(),
        P("gz", None, None),
        P("gz", None),
        P("ang", None, None),
        P("ang"),
    )
    out_specs = P(("gz", "ang"), None)
    return jax.shard_map(
        functools.partial(on_device, n_gz, n_ang),
        mesh=mesh, in_specs=in_specs, out_specs=out_specs, check_vma=False,
    )
```
